32 devices in a mesh: tm: 4 (over y, x), lat: 4 (over z), ens: 2 (over core).
Axes of the slice: x: 2, y: 2, z: 4, core: 2. Of those that a mesh axis runs over, the one named last changes fastest.
Arguments:
- increment: float32 [4, 4, 64, 1440], P('tm', None, 'lat'), may hold values from -6 to 6
- wind_lon: float32 [4, 4, 64, 1440], P('tm', None, 'lat'), may hold values from -0.45 to 0.45
- wind_lat: float32 [4, 4, 64, 1440], P('tm', None, 'lat'), may hold values from -0.45 to 0.45
- model_precision: float32 [4], replicated, may hold values from 0.5 to 4
- perturbations: float32 [32, 4, 64, 1440], P('ens', 'tm', 'lat'), may hold values from -0.24350093 to 0.24350093
- obs_rows: int32 [4, 128], P('tm', 'lat'), may hold values from 0 to 63
- obs_jacobian: float32 [4, 128, 16, 1440], P('tm', 'lat'), may hold values from -0.15625 to 0.15625
- obs_values: float32 [4, 128, 16], P('tm', 'lat'), may hold values from -6 to 6
- obs_precision: float32 [4, 128, 16], P('tm', 'lat'), may hold values from 0.5 to 2
- obs_counts: int32 [4, 128], P('tm', 'lat'), may hold values from 1 to 16
Outputs:
- grad_state: float32 [4, 4, 64, 1440], P('tm', None, 'lat')
- forcing_step: float32 [4, 64, 1440], P('tm', 'lat')
The draws below stay inside these ranges and needn't reach their ends.
Inputs may be any that keep to these rules, and one draw needn't show every extreme that they name: `obs_rows`: block j of band b reads level r // 16 and latitude b * 16 + r % 16, where r is its entry; several blocks may read the same row. `obs_counts`: only the first count slots of a block hold observations.
All inputs are finite; a program needn't handle non-finite values.
Results may differ from the reference program's by a relative error of at most 0.0003.
Values sent between devices are 32-bit elements; how exact they have to be, the bound alone decides.
A program may use at most 64 MiB of HBM per device.

```python
import math
import jax
import jax.numpy as jnp
from jax import lax

NLON = 1440
MEM = 32
CLAT = 16
STEPS = 4
OBS = 32
NOB = 16
NT = 4
LEV = 4
NLAT = 64
OBSALL = 128


def with_ends(entries, rng, least, top_value):
    longest = entries.shape.index(max(entries.shape))
    spots = []
    for shift in (0, 1):
        where = [jax.random.randint(jax.random.fold_in(rng, axis), (), 0, length) for axis, length in enumerate(entries.shape)]
        where[longest] = (where[longest] + shift) % entries.shape[longest]
        spots.append(tuple(where))
    return entries.at[spots[0]].set(least).at[spots[1]].set(top_value)


def shard_levels(own_key, extent, split, least, top_value):
    level = 1.0
    for axis_at, shards_of in split:
        draws = jax.random.uniform(jax.random.fold_in(jax.random.fold_in(own_key, 6), axis_at), (shards_of,), jnp.float32, least / len(split), top_value / len(split))
        level = level * jnp.repeat(jnp.exp(draws), extent[axis_at] // shards_of).reshape((-1,) + (1,) * (len(extent) - 1 - axis_at))
    return level


def noise(rng, extent, spread, most, pieces=(), kind=jnp.bfloat16):
    loudness = shard_levels(rng, extent, pieces, -0.22, 0.18) if pieces else 1.0
    entries = jax.random.normal(rng, extent, jnp.float32) * spread * loudness
    return jnp.minimum(jnp.maximum(entries, -most), most).astype(kind)


def setup_inputs(seed: int = 0) -> dict:
    arg_keys = jax.random.split(jax.random.key(seed), 11)
    return {
        "increment": noise(arg_keys[0], (NT, LEV, NLAT, NLON), 1.0, 6.0, ((0, 4), (2, 4)), jnp.float32),
        "wind_lon": jnp.clip(jax.random.uniform(arg_keys[1], (NT, LEV, NLAT, NLON), jnp.float32, -0.45, 0.45) * shard_levels(arg_keys[1], (NT, LEV, NLAT, NLON), ((0, 4), (2, 4)), -0.4, 0.0), -0.45, 0.45),
        "wind_lat": jnp.clip(jax.random.uniform(arg_keys[2], (NT, LEV, NLAT, NLON), jnp.float32, -0.45, 0.45) * shard_levels(arg_keys[2], (NT, LEV, NLAT, NLON), ((0, 4), (2, 4)), -0.4, 0.0), -0.45, 0.45),
        "model_precision": jnp.clip(jnp.exp(jax.random.uniform(arg_keys[3], (LEV,), jnp.float32, math.log(0.5), math.log(4.0))), 0.5, 4.0),
        "perturbations": noise(arg_keys[4], (MEM, LEV, NLAT, NLON), ((LEV * NLAT * NLON) ** -0.25), 0.24350093, ((0, 2), (1, 4), (2, 4)), jnp.float32),
        "obs_rows": with_ends(jax.random.randint(arg_keys[5], (NT, OBSALL), 0, LEV * CLAT), jax.random.fold_in(arg_keys[5], 1), 0, (LEV * CLAT) - 1).astype(jnp.int32),
        "obs_jacobian": noise(arg_keys[6], (NT, OBSALL, NOB, NLON), NLON ** -0.5, 0.15625, ((0, 4), (1, 4)), jnp.float32),
        "obs_values": noise(arg_keys[7], (NT, OBSALL, NOB), 1.0, 6.0, ((0, 4), (1, 4)), jnp.float32),
        "obs_precision": jnp.clip(jnp.exp(math.log(2.0) - 1.3862944 * jax.random.uniform(arg_keys[8], (NT, OBSALL, NOB), jnp.float32) ** shard_levels(arg_keys[8], (NT, OBSALL, NOB), ((0, 4), (1, 4)), -0.2, 0.2)), 0.5, 2.0),
        "obs_counts": with_ends(jax.random.randint(arg_keys[9], (NT, OBSALL), 1, NOB + 1), jax.random.fold_in(arg_keys[9], 1), 1, NOB).astype(jnp.int32),
    }


def coefficients(wind_lon, wind_lat):
    center = 1.0 - wind_lon * wind_lon - wind_lat * wind_lat
    plus_lon = 0.5 * (wind_lon * wind_lon - wind_lon)
    minus_lon = 0.5 * (wind_lon * wind_lon + wind_lon)
    plus_lat = 0.5 * (wind_lat * wind_lat - wind_lat)
    minus_lat = 0.5 * (wind_lat * wind_lat + wind_lat)
    return (center, plus_lon, minus_lon, plus_lat, minus_lat)


def advect(field, coefs):
    center, plus_lon, minus_lon, plus_lat, minus_lat = coefs
    northern = jnp.pad(field[:, 1:], ((0, 0), (0, 1), (0, 0)))
    southern = jnp.pad(field[:, :-1], ((0, 0), (1, 0), (0, 0)))
    return (center * field + plus_lon * jnp.roll(field, -1, 2) + minus_lon * jnp.roll(field, 1, 2)
            + plus_lat * northern + minus_lat * southern)


def advect_adjoint(field, coefs):
    center, plus_lon, minus_lon, plus_lat, minus_lat = coefs
    upward = plus_lat * field
    downward = minus_lat * field
    from_south = jnp.pad(upward[:, :-1], ((0, 0), (1, 0), (0, 0)))
    from_north = jnp.pad(downward[:, 1:], ((0, 0), (0, 1), (0, 0)))
    return (center * field + jnp.roll(plus_lon * field, 1, 2) + jnp.roll(minus_lon * field, -1, 2)
            + from_south + from_north)


def reference(increment, wind_lon, wind_lat, model_precision, perturbations, obs_rows, obs_jacobian,
              obs_values, obs_precision, obs_counts):
    highest = lax.Precision.HIGHEST
    level_prec = model_precision[:, None, None]
    band = jnp.arange(OBSALL, dtype=jnp.int32) // OBS
    slots = jnp.arange(NOB, dtype=jnp.int32)
    ends = []
    coef_list = []
    for window in range(NT):
        coefs = coefficients(wind_lon[window], wind_lat[window])
        coef_list.append(coefs)
        field = increment[window]
        for repeat in range(STEPS):
            field = advect(field, coefs)
        ends.append(field)
    mismatches = []
    for window in range(NT):
        if window > 0:
            mismatches.append(level_prec * (increment[window] - ends[window - 1]))
        else:
            mismatches.append(level_prec * increment[window])
    grads = []
    total = jnp.zeros((LEV, NLAT, NLON), jnp.float32)
    for window in range(NT):
        coefs = coef_list[window]
        rows = obs_rows[window].astype(jnp.int32)
        level = rows // CLAT
        latitude = band * CLAT + rows % CLAT
        picked = ends[window][level, latitude]
        jacobian = obs_jacobian[window]
        evolved = jnp.einsum('jon,jn->jo', jacobian, picked, precision=highest)
        used = (slots[None, :] < obs_counts[window][:, None]).astype(jnp.float32)
        weighted = obs_precision[window] * (evolved - obs_values[window]) * used
        force = jnp.einsum('jon,jo->jn', jacobian, weighted, precision=highest)
        adjoint = jnp.zeros((LEV, NLAT, NLON), jnp.float32).at[level, latitude].add(force)
        if window + 1 < NT:
            adjoint = adjoint - mismatches[window + 1]
        forcing = adjoint
        for repeat in range(STEPS):
            adjoint = advect_adjoint(adjoint, coefs)
            if repeat + 1 < STEPS:
                forcing = forcing + adjoint
        grads.append(adjoint + mismatches[window])
        total = total + forcing
    member_coef = jnp.einsum('mlan,lan->m', perturbations, total, precision=highest)
    forcing_step = -jnp.einsum('m,mlan->lan', member_coef, perturbations, precision=highest) / (MEM - 1.0)
    return jnp.stack(grads), forcing_step
```

```python
import functools

import jax
import jax.numpy as jnp
from jax import lax
from jax.experimental import pallas as pl
from jax.experimental.pallas import tpu as pltpu
from jax.sharding import PartitionSpec as P

STEPS = 4
MESH = pl.DeviceIdType.MESH
HIGHEST = lax.Precision.HIGHEST
NT = (((1,), (1,)), ((), ()))
NN = (((1,), (0,)), ((), ()))


def mm(a, b, dims, precision=None):
    return lax.dot_general(a, b, dims, precision=precision, preferred_element_type=jnp.float32)


def split(value):
    hi = value.astype(jnp.bfloat16)
    lo = (value - hi.astype(jnp.float32)).astype(jnp.bfloat16)
    return hi, lo


def turn(value, steps, axis):
    return pltpu.roll(value, steps % value.shape[axis], axis)


def extend(ref, where, lon):
    width = ref.shape[-1]
    rem = lon % 128
    last = ref[where + (slice(0, 16), slice(width - 128, width))]
    before = ref[where + (slice(0, 16), slice(width - 256, width - 128))]
    first = ref[where + (slice(0, 16), slice(0, 128))]
    lane = lax.broadcasted_iota(jnp.int32, last.shape, 1)
    wrapped = jnp.where(lane < 128 - rem, turn(before, 128 - rem, 1), turn(last, 128 - rem, 1))
    right = jnp.where(lane < rem + (128 - rem) // 2, turn(first, rem, 1), wrapped)
    ref[where + (slice(0, 16), slice(width - 128, width))] = jnp.where(lane < rem, last, right)


def pack(ref, lead, pair):
    one, two = lead + (2 * pair,), lead + (2 * pair + 1,)
    low = lax.broadcasted_iota(jnp.int32, (8, ref.shape[-1]), 0) < 4
    firsts = jnp.where(low, ref[one + (slice(0, 8),)], turn(ref[two + (slice(0, 8),)], 4, 0))
    lasts = jnp.where(low, turn(ref[one + (slice(8, 16),)], 4, 0), ref[two + (slice(8, 16),)])
    return firsts, lasts


def unpack(ref, lead, pair, after, before):
    low = lax.broadcasted_iota(jnp.int32, (8, ref.shape[-1]), 0) < 4
    ref[lead + (2 * pair, slice(16, 24))] = jnp.where(low, after, turn(before, 4, 0))
    ref[lead + (2 * pair + 1, slice(16, 24))] = jnp.where(low, turn(after, 4, 0), before)


def kernel(
    T, L, E,
    rows_ref, cnt_ref, val_ref, prc_ref, mp_ref, inc_hbm, wlon_hbm, wlat_hbm, jac_hbm, pert_hbm,
    grad_hbm, step_hbm,
    inc_v, wlon_v, wlat_v, jac_v, pert_v, jhi, jlo, wide, coef, adj,
    h_first, h_last, h_after, h_before, a_first, a_last, a_after, a_before,
    end_v, nxt_v, prior_v, forc, rs_v, ca_send, ca_v, cb_send, cb_v, grad_v, step_v,
    load_sem, h_ssem, h_rsem, a_ssem, a_rsem, t_ssem, t_rsem, p_ssem, p_rsem,
    rs_ssem, rs_rsem, ca_ssem, ca_rsem, cb_ssem, cb_rsem, g_ssem, g_rsem, out_sem,
):
    k, b, e = lax.axis_index("tm"), lax.axis_index("lat"), lax.axis_index("ens")
    half, crow, lon = inc_v.shape
    pairs = half // 2
    width = wide.shape[-1]
    members = pert_v.shape[1]
    blocks, slots = val_ref.shape
    flat = blocks * slots
    other = 1 - e
    own = pl.ds(e * half, half)

    loads = [
        pltpu.make_async_copy(inc_hbm.at[own], inc_v, load_sem.at[0]),
        pltpu.make_async_copy(wlon_hbm.at[own], wlon_v, load_sem.at[1]),
        pltpu.make_async_copy(wlat_hbm.at[own], wlat_v, load_sem.at[2]),
        pltpu.make_async_copy(jac_hbm, jac_v, load_sem.at[3]),
        pltpu.make_async_copy(pert_hbm, pert_v.at[e], load_sem.at[4]),
    ]
    for item in loads:
        item.start()

    barrier = pltpu.get_barrier_semaphore()
    group = [(dt, de) for dt in range(T) for de in range(E) if dt or de]

    def mate(dt, de):
        return {"tm": lax.rem(k + dt, T), "ens": lax.rem(e + de, E)}

    for dt, de in group:
        pl.semaphore_signal(barrier, inc=1, device_id=mate(dt, de), device_id_type=MESH)
    for db in range(1, L):
        pl.semaphore_signal(barrier, inc=1, device_id={"lat": lax.rem(b + db, L)}, device_id_type=MESH)

    def remote(src, dst, ssem, rsem, device):
        return pltpu.make_async_remote_copy(
            src_ref=src, dst_ref=dst, send_sem=ssem, recv_sem=rsem, device_id=device, device_id_type=MESH
        )

    up = {"lat": lax.rem(b + 1, L)}
    down = {"lat": lax.rem(b + L - 1, L)}
    later_dev = {"tm": lax.rem(k + 1, T)}
    prior_dev = {"tm": lax.rem(k + T - 1, T)}
    partner = {"ens": other}
    has_up, has_down = b < L - 1, b > 0
    has_later, has_prior = k < T - 1, k > 0

    for item in loads[:3]:
        item.wait()
    for at, ref in enumerate((inc_v, wlon_v, wlat_v)):
        for i in range(half):
            wide[at, i, 0:16, 0:lon] = ref[i]
            extend(wide, (at, i), lon)
        for pair in range(pairs):
            firsts, lasts = pack(wide, (at,), pair)
            h_first[at * pairs + pair] = firsts
            h_last[at * pairs + pair] = lasts

    pl.semaphore_wait(barrier, len(group) + L - 1)

    h_up = remote(h_last, h_before, h_ssem.at[0], h_rsem.at[0], up)
    h_down = remote(h_first, h_after, h_ssem.at[1], h_rsem.at[1], down)
    n_copy = remote(inc_v, nxt_v, t_ssem.at[0], t_rsem.at[0], prior_dev)

    @pl.when(has_up)
    def _():
        h_up.start()

    @pl.when(has_down)
    def _():
        h_down.start()

    @pl.when(has_prior)
    def _():
        n_copy.start()

    loads[4].wait()
    p_copy = remote(pert_v.at[e], pert_v.at[e], p_ssem, p_rsem, partner)
    p_copy.start()

    @pl.when(jnp.logical_not(has_up))
    def _():
        h_after[...] = jnp.zeros_like(h_after)
        a_after[...] = jnp.zeros_like(a_after)

    @pl.when(jnp.logical_not(has_down))
    def _():
        h_before[...] = jnp.zeros_like(h_before)
        a_before[...] = jnp.zeros_like(a_before)

    @pl.when(jnp.logical_not(has_prior))
    def _():
        prior_v[...] = jnp.zeros_like(prior_v)

    loads[3].wait()
    jhi[:, width - 128 : width] = jnp.zeros((flat, 128), jnp.bfloat16)
    jlo[:, width - 128 : width] = jnp.zeros((flat, 128), jnp.bfloat16)

    def cut(at, carry):
        some = pl.ds(pl.multiple_of(at * 32, 32), 32)
        hi, lo = split(jac_v[some, :])
        jhi[some, 0:lon] = hi
        jlo[some, 0:lon] = lo
        return carry

    lax.fori_loop(0, flat // 32, cut, 0)

    column = lax.broadcasted_iota(jnp.int32, (blocks, flat), 1)
    block = lax.broadcasted_iota(jnp.int32, (blocks, flat), 0)
    mine = (column >= block * slots) & (column < (block + 1) * slots)
    spread = mine.astype(jnp.float32)
    first_column = lax.broadcasted_iota(jnp.int32, (1, flat), 1)
    slot = (first_column % slots).astype(jnp.float32)
    tile_slot = lax.broadcasted_iota(jnp.int32, (slots, flat), 0)
    tile_column = lax.broadcasted_iota(jnp.int32, (slots, flat), 1) % slots
    tiled = (tile_slot == tile_column).astype(jnp.float32)

    def flatten(ref):
        return jnp.sum(mm(ref[...], tiled, NN, HIGHEST) * spread, axis=0, keepdims=True)

    values, precisions = flatten(val_ref), flatten(prc_ref)
    counts = mm(jnp.broadcast_to(cnt_ref[...].astype(jnp.float32), (8, blocks)), spread, NN, HIGHEST)[0:1]
    rows = mm(jnp.broadcast_to(rows_ref[...].astype(jnp.float32), (8, blocks)), spread, NN, HIGHEST)[0:1]
    precisions = jnp.where(slot < counts - 0.5, precisions, 0.0)
    local = lax.broadcasted_iota(jnp.int32, (half * crow, flat), 0) + e * (half * crow)
    reads = (jnp.abs(rows - local.astype(jnp.float32)) < 0.5).astype(jnp.float32)

    @pl.when(has_down)
    def _():
        h_up.wait_recv()

    @pl.when(has_up)
    def _():
        h_down.wait_recv()

    for at in range(3):
        for pair in range(pairs):
            slot_at = at * pairs + pair
            unpack(wide, (at,), pair, h_after[slot_at], h_before[slot_at])

    for i in range(half):
        wl, wt = wide[1, i], wide[2, i]
        wl2, wt2 = wl * wl, wt * wt
        coef[i, 0] = 1.0 - wl2 - wt2
        coef[i, 1] = 0.5 * (wl2 - wl)
        coef[i, 2] = 0.5 * (wl2 + wl)
        coef[i, 3] = 0.5 * (wt2 - wt)
        coef[i, 4] = 0.5 * (wt2 + wt)
        for _ in range(STEPS):
            f = wide[0, i]
            wide[0, i] = (
                coef[i, 0] * f
                + coef[i, 1] * turn(f, -1, 1)
                + coef[i, 2] * turn(f, 1, 1)
                + coef[i, 3] * turn(f, -1, 0)
                + coef[i, 4] * turn(f, 1, 0)
            )
        end_v[i] = wide[0, i, 0:crow]

    e_copy = remote(end_v, prior_v, t_ssem.at[1], t_rsem.at[1], later_dev)

    @pl.when(has_later)
    def _():
        e_copy.start()

    fhi, flo = split(jnp.concatenate([end_v[i] for i in range(half)], axis=0))
    jh, jl = jhi[...], jlo[...]
    seen = mm(fhi, jh, NT) + mm(flo, jh, NT) + mm(fhi, jl, NT)
    evolved = jnp.sum(seen * reads, axis=0, keepdims=True)
    whi, wlo = split(reads * (precisions * (evolved - values)))
    placed = mm(whi, jh, NN) + mm(wlo, jh, NN) + mm(whi, jl, NN)

    @pl.when(has_later)
    def _():
        n_copy.wait_recv()

    @pl.when(jnp.logical_not(has_later))
    def _():
        for i in range(half):
            nxt_v[i] = end_v[i, :, 0:lon]

    for i in range(half):
        prec = mp_ref[e * half + i]
        later = prec * (nxt_v[i] - end_v[i, :, 0:lon])
        adj[i, 0:crow, 0:lon] = placed[i * crow : (i + 1) * crow, 0:lon] - later
        extend(adj, (i,), lon)
    for pair in range(pairs):
        firsts, lasts = pack(adj, (), pair)
        a_first[pair] = firsts
        a_last[pair] = lasts
    a_up = remote(a_last, a_before, a_ssem.at[0], a_rsem.at[0], up)
    a_down = remote(a_first, a_after, a_ssem.at[1], a_rsem.at[1], down)

    @pl.when(has_up)
    def _():
        a_up.start()

    @pl.when(has_down)
    def _():
        a_down.start()

    @pl.when(has_down)
    def _():
        a_up.wait_recv()

    @pl.when(has_up)
    def _():
        a_down.wait_recv()

    for pair in range(pairs):
        unpack(adj, (), pair, a_after[pair], a_before[pair])

    def back(i):
        g = adj[i]
        return (
            coef[i, 0] * g
            + turn(coef[i, 1] * g, 1, 1)
            + turn(coef[i, 2] * g, -1, 1)
            + turn(coef[i, 3] * g, 1, 0)
            + turn(coef[i, 4] * g, -1, 0)
        )

    def owner_copy(i, h):
        return remote(
            forc.at[i, h], rs_v.at[k], rs_ssem.at[i, h], rs_rsem.at[k], {"tm": e * half + i, "ens": h}
        )

    for i in range(half):
        for h in range(E):
            forc[i, h] = adj[i, h * 8 : h * 8 + 8]
        for _ in range(STEPS - 1):
            adj[i] = back(i)
            for h in range(E):
                forc[i, h] += adj[i, h * 8 : h * 8 + 8]
        for h in range(E):
            here = (k == e * half + i) & (e == h)

            @pl.when(here)
            def _():
                rs_v[k] = forc[i, h]

            @pl.when(jnp.logical_not(here))
            def _():
                owner_copy(i, h).start()

    @pl.when(has_prior)
    def _():
        e_copy.wait_recv()

    for i in range(half):
        prec = mp_ref[e * half + i]
        g = back(i)
        grad_v[e * half + i] = g[0:crow, 0:lon] + prec * (inc_v[i] - prior_v[i, :, 0:lon])
    g_copy = remote(grad_v.at[own], grad_v.at[own], g_ssem, g_rsem, partner)
    g_copy.start()

    p_copy.wait_recv()
    for at in range(T):
        inside = (k == at) & (e == at // half)

        @pl.when(jnp.logical_not(inside))
        def _():
            remote(forc.at[0, 0], rs_v.at[at], rs_ssem.at[0, 0], rs_rsem.at[at], partner).wait_recv()

    total = rs_v[0]
    for at in range(1, T):
        total = total + rs_v[at]
    total = total[:, 0:lon]
    lane = lax.broadcasted_iota(jnp.int32, (8, 128), 1)
    part = jnp.zeros((8, 128), jnp.float32)
    for m in range(E * members):
        dots = jnp.sum(pert_v[m // members, m % members, e] * total, axis=1, keepdims=True)
        part = jnp.where(lane == m, dots, part)
    ca_send[...] = part
    me = k * E + e
    ca_v[me] = part
    ca_copies = []
    for dt, de in group:
        copy = remote(ca_send, ca_v.at[me], ca_ssem.at[dt * E + de], ca_rsem.at[me], mate(dt, de))
        copy.start()
        ca_copies.append(copy)
    for dt, de in group:
        it = lax.rem(k + dt, T) * E + lax.rem(e + de, E)
        remote(ca_send, ca_v.at[it], ca_ssem.at[0], ca_rsem.at[it], partner).wait_recv()
    part = ca_v[0]
    for at in range(1, T * E):
        part = part + ca_v[at]
    cb_send[...] = part
    cb_v[b] = part
    cb_copies = []
    for db in range(1, L):
        copy = remote(cb_send, cb_v.at[b], cb_ssem.at[db], cb_rsem.at[b], {"lat": lax.rem(b + db, L)})
        copy.start()
        cb_copies.append(copy)

    g_copy.wait_recv()
    g_out = pltpu.make_async_copy(grad_v, grad_hbm, out_sem.at[0])
    g_out.start()

    for db in range(1, L):
        it = lax.rem(b + db, L)
        remote(cb_send, cb_v.at[it], cb_ssem.at[0], cb_rsem.at[it], partner).wait_recv()
    part = cb_v[0]
    for at in range(1, L):
        part = part + cb_v[at]
    factor = jnp.broadcast_to(jnp.sum(part, axis=0, keepdims=True), (8, 128)) * (-1.0 / (E * members - 1.0))
    for h in range(crow // 8):
        mixed = jnp.zeros((8, lon), jnp.float32)
        for m in range(E * members):
            mixed = mixed + factor[:, m : m + 1] * pert_v[m // members, m % members, h]
        step_v[h * 8 : h * 8 + 8, :] = mixed
    s_out = pltpu.make_async_copy(step_v, step_hbm, out_sem.at[1])
    s_out.start()

    @pl.when(has_up)
    def _():
        h_up.wait_send()
        a_up.wait_send()

    @pl.when(has_down)
    def _():
        h_down.wait_send()
        a_down.wait_send()

    @pl.when(has_prior)
    def _():
        n_copy.wait_send()

    @pl.when(has_later)
    def _():
        e_copy.wait_send()

    p_copy.wait_send()
    g_copy.wait_send()
    for i in range(half):
        for h in range(E):
            here = (k == e * half + i) & (e == h)

            @pl.when(jnp.logical_not(here))
            def _():
                owner_copy(i, h).wait_send()

    for copy in ca_copies + cb_copies:
        copy.wait_send()
    g_out.wait()
    s_out.wait()


def on_device(T, L, E, increment, wind_lon, wind_lat, model_precision, perturbations, obs_rows, obs_jacobian,
              obs_values, obs_precision, obs_counts):
    _, levels, crow, lon = increment.shape
    members = perturbations.shape[0]
    blocks, slots = obs_jacobian.shape[1:3]
    half, width = levels // E, -(-lon // 128) * 128
    pairs, flat = half // 2, blocks * slots
    f32, dma = jnp.float32, pltpu.SemaphoreType.DMA
    vmem, anyw = pl.BlockSpec(memory_space=pltpu.VMEM), pl.BlockSpec(memory_space=pl.ANY)

    def buf(*shape, kind=f32):
        return pltpu.VMEM(shape, kind)

    grad, step = pl.pallas_call(
        functools.partial(kernel, T, L, E),
        out_shape=(
            jax.ShapeDtypeStruct((levels, crow, lon), f32),
            jax.ShapeDtypeStruct((crow, lon), f32),
        ),
        in_specs=[vmem] * 4 + [pl.BlockSpec(memory_space=pltpu.SMEM)] + [anyw] * 5,
        out_specs=(anyw, anyw),
        scratch_shapes=[
            buf(half, crow, lon), buf(half, crow, lon), buf(half, crow, lon),
            buf(flat, lon), buf(E, members, crow // 8, 8, lon),
            buf(flat, width, kind=jnp.bfloat16), buf(flat, width, kind=jnp.bfloat16),
            buf(3, half, 24, width), buf(half, 5, 24, width), buf(half, 24, width),
            buf(3 * pairs, 8, width), buf(3 * pairs, 8, width), buf(3 * pairs, 8, width), buf(3 * pairs, 8, width),
            buf(pairs, 8, width), buf(pairs, 8, width), buf(pairs, 8, width), buf(pairs, 8, width),
            buf(half, crow, width), buf(half, crow, lon), buf(half, crow, width),
            buf(half, E, 8, width), buf(T, 8, width),
            buf(8, 128), buf(T * E, 8, 128), buf(8, 128), buf(L, 8, 128),
            buf(levels, crow, lon), buf(crow, lon),
            dma((5,)), dma((2,)), dma((2,)), dma((2,)), dma((2,)), dma((2,)), dma((2,)), dma, dma,
            dma((half, E)), dma((T,)), dma((T * E,)), dma((T * E,)), dma((L,)), dma((L,)), dma, dma, dma((2,)),
        ],
        compiler_params=pltpu.CompilerParams(
            collective_id=0, has_side_effects=True, vmem_limit_bytes=60 * 1024 * 1024
        ),
    )(
        obs_rows, obs_counts, obs_values[0], obs_precision[0], model_precision,
        increment[0], wind_lon[0], wind_lat[0],
        obs_jacobian.reshape(flat, lon),
        perturbations.reshape(members, crow // 8, 8, lon),
    )
    return grad[None], step[None]


def solution(mesh):
    T, L, E = mesh.shape["tm"], mesh.shape["lat"], mesh.shape["ens"]
    placed = (
        P("tm", None, "lat", None),
        P("tm", None, "lat", None),
        P("tm", None, "lat", None),
        P(),
        P("ens", "tm", "lat", None),
        P("tm", "lat"),
        P("tm", "lat", None, None),
        P("tm", "lat", None),
        P("tm", "lat", None),
        P("tm", "lat"),
    )
    return jax.shard_map(
        functools.partial(on_device, T, L, E),
        mesh=mesh,
        in_specs=placed,
        out_specs=(P("tm", None, "lat", None), P("tm", "lat", None)),
        check_vma=False,
    )
```

```python
import functools

import jax
import jax.numpy as jnp
from jax import lax
from jax.experimental import pallas as pl
from jax.experimental.pallas import tpu as pltpu
from jax.sharding import PartitionSpec as P

STEPS = 4
MESH = pl.DeviceIdType.MESH
HIGHEST = lax.Precision.HIGHEST
NT = (((1,), (1,)), ((), ()))
NN = (((1,), (0,)), ((), ()))


def mm(a, b, dims, precision=None):
    return lax.dot_general(a, b, dims, precision=precision, preferred_element_type=jnp.float32)


def split(value):
    hi = value.astype(jnp.bfloat16)
    lo = (value - hi.astype(jnp.float32)).astype(jnp.bfloat16)
    return hi, lo


def turn(value, steps, axis):
    return pltpu.roll(value, steps % value.shape[axis], axis)


def extend(ref, where, lon):
    width = ref.shape[-1]
    rem = lon % 128
    last = ref[where + (slice(0, 16), slice(width - 128, width))]
    before = ref[where + (slice(0, 16), slice(width - 256, width - 128))]
    first = ref[where + (slice(0, 16), slice(0, 128))]
    lane = lax.broadcasted_iota(jnp.int32, last.shape, 1)
    wrapped = jnp.where(lane < 128 - rem, turn(before, 128 - rem, 1), turn(last, 128 - rem, 1))
    right = jnp.where(lane < rem + (128 - rem) // 2, turn(first, rem, 1), wrapped)
    ref[where + (slice(0, 16), slice(width - 128, width))] = jnp.where(lane < rem, last, right)


def pack(ref, lead, pair):
    one, two = lead + (2 * pair,), lead + (2 * pair + 1,)
    low = lax.broadcasted_iota(jnp.int32, (8, ref.shape[-1]), 0) < 4
    firsts = jnp.where(low, ref[one + (slice(0, 8),)], turn(ref[two + (slice(0, 8),)], 4, 0))
    lasts = jnp.where(low, turn(ref[one + (slice(8, 16),)], 4, 0), ref[two + (slice(8, 16),)])
    return firsts, lasts


def unpack(ref, lead, pair, after, before):
    low = lax.broadcasted_iota(jnp.int32, (8, ref.shape[-1]), 0) < 4
    ref[lead + (2 * pair, slice(16, 24))] = jnp.where(low, after, turn(before, 4, 0))
    ref[lead + (2 * pair + 1, slice(16, 24))] = jnp.where(low, turn(after, 4, 0), before)


def kernel(
    T, L, E,
    rows_hbm, cnt_hbm, val_hbm, prc_hbm, mp_hbm, inc_hbm, wlon_hbm, wlat_hbm, jac_hbm, pert_hbm,
    grad_v, pert_v, cb_v,
    rows_ref, cnt_ref, val_ref, prc_ref, mp_ref, inc_v, wlon_v, wlat_v, jac_v, jhi, jlo, wide, coef, adj,
    h_first, h_last, h_after, h_before, a_up_v, a_down_v, a_after, a_before,
    end_v, nxt_v, prior_v, forc, edge, rs_v, edge_v, ca_send, ca_v, cb_send,
    load_sem, h_ssem, h_rsem, a_ssem, a_rsem, t_ssem, t_rsem, p_ssem, p_rsem,
    rs_ssem, rs_rsem, ed_ssem, ed_rsem, ca_ssem, ca_rsem, cb_ssem, cb_rsem, g_ssem, g_rsem,
):
    k, b, e = lax.axis_index("tm"), lax.axis_index("lat"), lax.axis_index("ens")
    half, crow, lon = inc_v.shape
    pairs = half // 2
    width = wide.shape[-1]
    members = pert_v.shape[1]
    slots, blocks = val_ref.shape
    flat = blocks * slots
    other = 1 - e
    own = pl.ds(e * half, half)

    loads = [
        pltpu.make_async_copy(inc_hbm.at[own], inc_v, load_sem.at[0]),
        pltpu.make_async_copy(wlon_hbm.at[own], wlon_v, load_sem.at[1]),
        pltpu.make_async_copy(wlat_hbm.at[own], wlat_v, load_sem.at[2]),
        pltpu.make_async_copy(jac_hbm, jac_v, load_sem.at[3]),
        pltpu.make_async_copy(pert_hbm, pert_v.at[e], load_sem.at[4]),
        pltpu.make_async_copy(rows_hbm, rows_ref, load_sem.at[5]),
        pltpu.make_async_copy(cnt_hbm, cnt_ref, load_sem.at[6]),
        pltpu.make_async_copy(val_hbm, val_ref, load_sem.at[7]),
        pltpu.make_async_copy(prc_hbm, prc_ref, load_sem.at[8]),
        pltpu.make_async_copy(mp_hbm, mp_ref, load_sem.at[9]),
    ]
    for item in loads:
        item.start()

    barrier = pltpu.get_barrier_semaphore()
    group = [(dt, de) for dt in range(T) for de in range(E) if dt or de]

    def mate(dt, de):
        return {"tm": lax.rem(k + dt, T), "ens": lax.rem(e + de, E)}

    for dt, de in group:
        pl.semaphore_signal(barrier, inc=1, device_id=mate(dt, de), device_id_type=MESH)
    for db in range(1, L):
        pl.semaphore_signal(barrier, inc=1, device_id={"lat": lax.rem(b + db, L)}, device_id_type=MESH)

    def remote(src, dst, ssem, rsem, device):
        return pltpu.make_async_remote_copy(
            src_ref=src, dst_ref=dst, send_sem=ssem, recv_sem=rsem, device_id=device, device_id_type=MESH
        )

    up = {"lat": lax.rem(b + 1, L)}
    down = {"lat": lax.rem(b + L - 1, L)}
    later_dev = {"tm": lax.rem(k + 1, T)}
    prior_dev = {"tm": lax.rem(k + T - 1, T)}
    partner = {"ens": other}
    has_up, has_down = b < L - 1, b > 0
    has_later, has_prior = k < T - 1, k > 0

    for item in loads[:3]:
        item.wait()
    for at, ref in enumerate((inc_v, wlon_v, wlat_v)):
        for i in range(half):
            wide[at, i, 0:16, 0:lon] = ref[i]
            extend(wide, (at, i), lon)
        for pair in range(pairs):
            firsts, lasts = pack(wide, (at,), pair)
            h_first[at * pairs + pair] = firsts
            h_last[at * pairs + pair] = lasts

    pl.semaphore_wait(barrier, len(group) + L - 1)

    h_up = remote(h_last, h_before, h_ssem.at[0], h_rsem.at[0], up)
    h_down = remote(h_first, h_after, h_ssem.at[1], h_rsem.at[1], down)
    n_copy = remote(inc_v, nxt_v, t_ssem.at[0], t_rsem.at[0], prior_dev)

    @pl.when(has_up)
    def _():
        h_up.start()

    @pl.when(has_down)
    def _():
        h_down.start()

    @pl.when(has_prior)
    def _():
        n_copy.start()

    loads[4].wait()
    p_copy = remote(pert_v.at[e], pert_v.at[e], p_ssem, p_rsem, partner)
    p_copy.start()

    @pl.when(jnp.logical_not(has_up))
    def _():
        h_after[...] = jnp.zeros_like(h_after)
        a_after[...] = jnp.zeros_like(a_after)

    @pl.when(jnp.logical_not(has_down))
    def _():
        h_before[...] = jnp.zeros_like(h_before)
        a_before[...] = jnp.zeros_like(a_before)

    @pl.when(jnp.logical_not(has_prior))
    def _():
        prior_v[...] = jnp.zeros_like(prior_v)

    edge_in = ((e == 0) & has_down) | ((e == E - 1) & has_up)

    @pl.when(jnp.logical_not(edge_in))
    def _():
        edge_v[...] = jnp.zeros_like(edge_v)

    for item in loads[5:]:
        item.wait()
    loads[3].wait()
    jhi[:, width - 128 : width] = jnp.zeros((flat, 128), jnp.bfloat16)
    jlo[:, width - 128 : width] = jnp.zeros((flat, 128), jnp.bfloat16)

    def cut(at, carry):
        some = pl.ds(pl.multiple_of(at * 32, 32), 32)
        hi, lo = split(jac_v[some, :])
        jhi[some, 0:lon] = hi
        jlo[some, 0:lon] = lo
        return carry

    lax.fori_loop(0, flat // 32, cut, 0)

    column = lax.broadcasted_iota(jnp.int32, (blocks, flat), 1)
    block = lax.broadcasted_iota(jnp.int32, (blocks, flat), 0)
    mine = (column >= block * slots) & (column < (block + 1) * slots)
    spread = mine.astype(jnp.float32)
    first_column = lax.broadcasted_iota(jnp.int32, (1, flat), 1)
    slot = (first_column % slots).astype(jnp.float32)
    tile_slot = lax.broadcasted_iota(jnp.int32, (slots, flat), 0)
    tile_column = lax.broadcasted_iota(jnp.int32, (slots, flat), 1) % slots
    tiled = (tile_slot == tile_column).astype(jnp.float32)

    def flatten(ref):
        return jnp.sum(mm(ref[...], spread, NN, HIGHEST) * tiled, axis=0, keepdims=True)

    values, precisions = flatten(val_ref), flatten(prc_ref)
    counts = mm(jnp.broadcast_to(cnt_ref[...].astype(jnp.float32), (8, blocks)), spread, NN, HIGHEST)[0:1]
    rows = mm(jnp.broadcast_to(rows_ref[...].astype(jnp.float32), (8, blocks)), spread, NN, HIGHEST)[0:1]
    precisions = jnp.where(slot < counts - 0.5, precisions, 0.0)
    local = lax.broadcasted_iota(jnp.int32, (half * crow, flat), 0) + e * (half * crow)
    reads = (jnp.abs(rows - local.astype(jnp.float32)) < 0.5).astype(jnp.float32)

    @pl.when(has_down)
    def _():
        h_up.wait_recv()

    @pl.when(has_up)
    def _():
        h_down.wait_recv()

    for at in range(3):
        for pair in range(pairs):
            slot_at = at * pairs + pair
            unpack(wide, (at,), pair, h_after[slot_at], h_before[slot_at])

    for i in range(half):
        wl, wt = wide[1, i], wide[2, i]
        wl2, wt2 = wl * wl, wt * wt
        coef[i, 0] = 1.0 - wl2 - wt2
        coef[i, 1] = 0.5 * (wl2 - wl)
        coef[i, 2] = 0.5 * (wl2 + wl)
        coef[i, 3] = 0.5 * (wt2 - wt)
        coef[i, 4] = 0.5 * (wt2 + wt)
        for _ in range(STEPS):
            f = wide[0, i]
            wide[0, i] = (
                coef[i, 0] * f
                + coef[i, 1] * turn(f, -1, 1)
                + coef[i, 2] * turn(f, 1, 1)
                + coef[i, 3] * turn(f, -1, 0)
                + coef[i, 4] * turn(f, 1, 0)
            )
        end_v[i] = wide[0, i, 0:crow]

    e_copy = remote(end_v, prior_v, t_ssem.at[1], t_rsem.at[1], later_dev)

    @pl.when(has_later)
    def _():
        e_copy.start()

    fhi, flo = split(jnp.concatenate([end_v[i] for i in range(half)], axis=0))
    jh, jl = jhi[...], jlo[...]
    seen = mm(fhi, jh, NT) + mm(flo, jh, NT) + mm(fhi, jl, NT)
    evolved = jnp.sum(seen * reads, axis=0, keepdims=True)
    whi, wlo = split(reads * (precisions * (evolved - values)))
    placed = mm(whi, jh, NN) + mm(wlo, jh, NN) + mm(whi, jl, NN)

    @pl.when(has_later)
    def _():
        n_copy.wait_recv()

    @pl.when(jnp.logical_not(has_later))
    def _():
        for i in range(half):
            nxt_v[i] = end_v[i, :, 0:lon]

    for i in range(half):
        prec = mp_ref[e * half + i]
        later = prec * (nxt_v[i] - end_v[i, :, 0:lon])
        adj[i, 0:crow, 0:lon] = placed[i * crow : (i + 1) * crow, 0:lon] - later
        extend(adj, (i,), lon)
        adj[i, crow : crow + 8] = jnp.zeros((8, width), jnp.float32)

    def back(i):
        g = adj[i]
        return (
            coef[i, 0] * g
            + turn(coef[i, 1] * g, 1, 1)
            + turn(coef[i, 2] * g, -1, 1)
            + turn(coef[i, 3] * g, 1, 0)
            + turn(coef[i, 4] * g, -1, 0)
        )

    def owner_copy(i, h):
        return remote(
            forc.at[i, h], rs_v.at[k], rs_ssem.at[i, h], rs_rsem.at[k], {"tm": e * half + i, "ens": h}
        )

    def edge_copy(i, h, device):
        return remote(edge.at[i, h], edge_v.at[k], ed_ssem.at[i, h], ed_rsem.at[k], device)

    edge_up = [edge_copy(i, 0, {"tm": e * half + i, "lat": lax.rem(b + 1, L), "ens": 0}) for i in range(half)]
    edge_down = [
        edge_copy(i, 1, {"tm": e * half + i, "lat": lax.rem(b + L - 1, L), "ens": E - 1}) for i in range(half)
    ]

    for i in range(half):
        for h in range(E):
            forc[i, h] = adj[i, h * 8 : h * 8 + 8]
        rim = jnp.zeros((8, width), jnp.float32)
        for _ in range(STEPS - 1):
            adj[i] = back(i)
            for h in range(E):
                forc[i, h] += adj[i, h * 8 : h * 8 + 8]
            rim = rim + adj[i, crow : crow + 8]
        edge[i, 0] = rim[0:4]
        edge[i, 1] = rim[4:8]

        @pl.when(has_up)
        def _():
            edge_up[i].start()

        @pl.when(has_down)
        def _():
            edge_down[i].start()

        for h in range(E):
            here = (k == e * half + i) & (e == h)

            @pl.when(here)
            def _():
                rs_v[k] = forc[i, h]

            @pl.when(jnp.logical_not(here))
            def _():
                owner_copy(i, h).start()

    for i in range(half):
        adj[i] = back(i)
        a_up_v[i] = adj[i, crow : crow + 4]
        a_down_v[i] = adj[i, crow + 4 : crow + 8]
    a_up = remote(a_up_v, a_before, a_ssem.at[0], a_rsem.at[0], up)
    a_down = remote(a_down_v, a_after, a_ssem.at[1], a_rsem.at[1], down)

    @pl.when(has_up)
    def _():
        a_up.start()

    @pl.when(has_down)
    def _():
        a_down.start()

    @pl.when(has_prior)
    def _():
        e_copy.wait_recv()

    @pl.when(has_down)
    def _():
        a_up.wait_recv()

    @pl.when(has_up)
    def _():
        a_down.wait_recv()

    for i in range(half):
        prec = mp_ref[e * half + i]
        gap = jnp.zeros((crow - 8, lon), jnp.float32)
        rims = jnp.concatenate([a_before[i][:, 0:lon], gap, a_after[i][:, 0:lon]], axis=0)
        grad_v[e * half + i] = adj[i, 0:crow, 0:lon] + rims + prec * (inc_v[i] - prior_v[i, :, 0:lon])
    g_copy = remote(grad_v.at[own], grad_v.at[own], g_ssem, g_rsem, partner)
    g_copy.start()

    p_copy.wait_recv()
    for at in range(T):
        inside = (k == at) & (e == at // half)

        @pl.when(jnp.logical_not(inside))
        def _():
            remote(forc.at[0, 0], rs_v.at[at], rs_ssem.at[0, 0], rs_rsem.at[at], partner).wait_recv()

    @pl.when(edge_in)
    def _():
        for at in range(T):
            remote(edge.at[0, 0], edge_v.at[at], ed_ssem.at[0, 0], ed_rsem.at[at], partner).wait_recv()

    total, rim = rs_v[0], edge_v[0]
    for at in range(1, T):
        total = total + rs_v[at]
        rim = rim + edge_v[at]
    line = lax.broadcasted_iota(jnp.int32, (8, width), 0)
    rim = jnp.concatenate([rim, rim], axis=0)
    total = total + jnp.where((line < 4) == (e == 0), rim, 0.0)
    total = total[:, 0:lon]
    lane = lax.broadcasted_iota(jnp.int32, (8, 128), 1)
    part = jnp.zeros((8, 128), jnp.float32)
    for m in range(E * members):
        dots = jnp.sum(pert_v[m // members, m % members, e] * total, axis=1, keepdims=True)
        part = jnp.where(lane == m, dots, part)
    ca_send[...] = part
    me = k * E + e
    ca_v[me] = part
    ca_copies = []
    for dt, de in group:
        copy = remote(ca_send, ca_v.at[me], ca_ssem.at[dt * E + de], ca_rsem.at[me], mate(dt, de))
        copy.start()
        ca_copies.append(copy)
    for dt, de in group:
        it = lax.rem(k + dt, T) * E + lax.rem(e + de, E)
        remote(ca_send, ca_v.at[it], ca_ssem.at[0], ca_rsem.at[it], partner).wait_recv()
    part = ca_v[0]
    for at in range(1, T * E):
        part = part + ca_v[at]
    cb_send[...] = part
    cb_v[b] = part
    cb_copies = []
    for db in range(1, L):
        copy = remote(cb_send, cb_v.at[b], cb_ssem.at[db], cb_rsem.at[b], {"lat": lax.rem(b + db, L)})
        copy.start()
        cb_copies.append(copy)

    g_copy.wait_recv()
    for db in range(1, L):
        it = lax.rem(b + db, L)
        remote(cb_send, cb_v.at[it], cb_ssem.at[0], cb_rsem.at[it], partner).wait_recv()
    @pl.when(has_up)
    def _():
        h_up.wait_send()
        a_up.wait_send()

    @pl.when(has_down)
    def _():
        h_down.wait_send()
        a_down.wait_send()

    @pl.when(has_prior)
    def _():
        n_copy.wait_send()

    @pl.when(has_later)
    def _():
        e_copy.wait_send()

    p_copy.wait_send()
    g_copy.wait_send()
    for i in range(half):
        for h in range(E):
            here = (k == e * half + i) & (e == h)

            @pl.when(jnp.logical_not(here))
            def _():
                owner_copy(i, h).wait_send()

    for i in range(half):
        @pl.when(has_up)
        def _():
            edge_up[i].wait_send()

        @pl.when(has_down)
        def _():
            edge_down[i].wait_send()

    for copy in ca_copies + cb_copies:
        copy.wait_send()


def finish(L, grad_v, pert_v, cb_v, grad_hbm, step_hbm, step_v, out_sem):
    g_out = pltpu.make_async_copy(grad_v, grad_hbm, out_sem.at[0])
    g_out.start()
    ens, members, rows, _, lon = pert_v.shape
    count = ens * members
    part = cb_v[0]
    for at in range(1, L):
        part = part + cb_v[at]
    factor = jnp.broadcast_to(jnp.sum(part, axis=0, keepdims=True), (8, 128)) * (-1.0 / (count - 1.0))
    for h in range(rows):
        mixed = jnp.zeros((8, lon), jnp.float32)
        for m in range(count):
            mixed = mixed + factor[:, m : m + 1] * pert_v[m // members, m % members, h]
        step_v[h * 8 : h * 8 + 8, :] = mixed
    s_out = pltpu.make_async_copy(step_v, step_hbm, out_sem.at[1])
    s_out.start()
    g_out.wait()
    s_out.wait()


def on_device(T, L, E, increment, wind_lon, wind_lat, model_precision, perturbations, obs_rows, obs_jacobian,
              obs_values, obs_precision, obs_counts):
    _, levels, crow, lon = increment.shape
    members = perturbations.shape[0]
    blocks, slots = obs_jacobian.shape[1:3]
    half, width = levels // E, -(-lon // 128) * 128
    pairs, flat = half // 2, blocks * slots
    f32, dma = jnp.float32, pltpu.SemaphoreType.DMA
    vmem, anyw = pl.BlockSpec(memory_space=pltpu.VMEM), pl.BlockSpec(memory_space=pl.ANY)

    def buf(*shape, kind=f32):
        return pltpu.VMEM(shape, kind)

    parts = pl.pallas_call(
        functools.partial(kernel, T, L, E),
        out_shape=(
            buf(levels, crow, lon),
            buf(E, members, crow // 8, 8, lon),
            buf(L, 8, 128),
        ),
        in_specs=[pl.BlockSpec(memory_space=pltpu.HBM)] * 10,
        out_specs=(vmem, vmem, vmem),
        scratch_shapes=[
            pltpu.VMEM((1, blocks), jnp.int32), pltpu.VMEM((1, blocks), jnp.int32),
            buf(slots, blocks), buf(slots, blocks), pltpu.SMEM((levels,), f32),
            buf(half, crow, lon), buf(half, crow, lon), buf(half, crow, lon),
            buf(flat, lon),
            buf(flat, width, kind=jnp.bfloat16), buf(flat, width, kind=jnp.bfloat16),
            buf(3, half, 24, width), buf(half, 5, 24, width), buf(half, 24, width),
            buf(3 * pairs, 8, width), buf(3 * pairs, 8, width), buf(3 * pairs, 8, width), buf(3 * pairs, 8, width),
            buf(half, 4, width), buf(half, 4, width), buf(half, 4, width), buf(half, 4, width),
            buf(half, crow, width), buf(half, crow, lon), buf(half, crow, width),
            buf(half, E, 8, width), buf(half, 2, 4, width), buf(T, 8, width), buf(T, 4, width),
            buf(8, 128), buf(T * E, 8, 128), buf(8, 128),
            dma((10,)), dma((2,)), dma((2,)), dma((2,)), dma((2,)), dma((2,)), dma((2,)), dma, dma,
            dma((half, E)), dma((T,)), dma((half, 2)), dma((T,)),
            dma((T * E,)), dma((T * E,)), dma((L,)), dma((L,)), dma, dma,
        ],
        compiler_params=pltpu.CompilerParams(
            collective_id=0, has_side_effects=True, vmem_limit_bytes=56 * 1024 * 1024
        ),
    )(
        obs_rows, obs_counts, obs_values[0].T, obs_precision[0].T, model_precision,
        increment[0], wind_lon[0], wind_lat[0],
        obs_jacobian.reshape(flat, lon),
        perturbations.reshape(members, crow // 8, 8, lon),
    )
    grad, step = pl.pallas_call(
        functools.partial(finish, L),
        out_shape=(
            jax.ShapeDtypeStruct((levels, crow, lon), f32),
            jax.ShapeDtypeStruct((crow, lon), f32),
        ),
        in_specs=[vmem] * 3,
        out_specs=(anyw, anyw),
        scratch_shapes=[buf(crow, lon), dma((2,))],
        compiler_params=pltpu.CompilerParams(vmem_limit_bytes=8 * 1024 * 1024),
    )(*[pltpu.with_memory_space_constraint(item, pltpu.VMEM) for item in parts])
    return grad[None], step[None]


def solution(mesh):
    T, L, E = mesh.shape["tm"], mesh.shape["lat"], mesh.shape["ens"]
    placed = (
        P("tm", None, "lat", None),
        P("tm", None, "lat", None),
        P("tm", None, "lat", None),
        P(),
        P("ens", "tm", "lat", None),
        P("tm", "lat"),
        P("tm", "lat", None, None),
        P("tm", "lat", None),
        P("tm", "lat", None),
        P("tm", "lat"),
    )
    return jax.shard_map(
        functools.partial(on_device, T, L, E),
        mesh=mesh,
        in_specs=placed,
        out_specs=(P("tm", None, "lat", None), P("tm", "lat", None)),
        check_vma=False,
    )
```

```python
import functools

import jax
import jax.numpy as jnp
from jax import lax
from jax.experimental import pallas as pl
from jax.experimental.pallas import tpu as pltpu
from jax.sharding import PartitionSpec as P

STEPS = 4
MESH = pl.DeviceIdType.MESH
HIGHEST = lax.Precision.HIGHEST
NT = (((1,), (1,)), ((), ()))
NN = (((1,), (0,)), ((), ()))


def mm(a, b, dims, precision=None):
    return lax.dot_general(a, b, dims, precision=precision, preferred_element_type=jnp.float32)


def split(value):
    hi = value.astype(jnp.bfloat16)
    lo = (value - hi.astype(jnp.float32)).astype(jnp.bfloat16)
    return hi, lo


def turn(value, steps, axis):
    return pltpu.roll(value, steps % value.shape[axis], axis)


def extend(ref, where, lon):
    width = ref.shape[-1]
    rem = lon % 128
    last = ref[where + (slice(0, 16), slice(width - 128, width))]
    before = ref[where + (slice(0, 16), slice(width - 256, width - 128))]
    first = ref[where + (slice(0, 16), slice(0, 128))]
    lane = lax.broadcasted_iota(jnp.int32, last.shape, 1)
    wrapped = jnp.where(lane < 128 - rem, turn(before, 128 - rem, 1), turn(last, 128 - rem, 1))
    right = jnp.where(lane < rem + (128 - rem) // 2, turn(first, rem, 1), wrapped)
    ref[where + (slice(0, 16), slice(width - 128, width))] = jnp.where(lane < rem, last, right)


def kernel(
    T, L, E,
    rows_hbm, cnt_hbm, val_hbm, prc_hbm, mp_hbm, inc_hbm, wlon_hbm, wlat_hbm, jac_hbm, pert_hbm,
    grad_v, pert_v, cb_v,
    rows_ref, cnt_ref, val_ref, prc_ref, mp_ref, inc_v, wlon_v, wlat_v, jac_v, jhi, jlo, wide, coef, adj,
    h_first, h_last, h_after, h_before, a_up_v, a_down_v, a_after, a_before,
    end_v, nxt_v, prior_v, forc, edge, rs_v, edge_v, ca_send, ca_v, cb_send,
    load_sem, h_ssem, h_rsem, a_ssem, a_rsem, t_ssem, t_rsem, e_ssem, e_rsem, p_ssem, p_rsem,
    rs_ssem, rs_rsem, ed_ssem, ed_rsem, ca_ssem, ca_rsem, cb_ssem, cb_rsem, g_ssem, g_rsem,
):
    k, b, e = lax.axis_index("tm"), lax.axis_index("lat"), lax.axis_index("ens")
    half, crow, lon = inc_v.shape
    width = wide.shape[-1]
    members = pert_v.shape[1]
    slots, blocks = val_ref.shape
    flat = blocks * slots
    other = 1 - e
    own = pl.ds(e * half, half)

    loads = [
        pltpu.make_async_copy(inc_hbm.at[own], inc_v, load_sem.at[0]),
        pltpu.make_async_copy(wlon_hbm.at[own], wlon_v, load_sem.at[1]),
        pltpu.make_async_copy(wlat_hbm.at[own], wlat_v, load_sem.at[2]),
        pltpu.make_async_copy(jac_hbm, jac_v, load_sem.at[3]),
        pltpu.make_async_copy(pert_hbm, pert_v.at[e], load_sem.at[4]),
        pltpu.make_async_copy(rows_hbm, rows_ref, load_sem.at[5]),
        pltpu.make_async_copy(cnt_hbm, cnt_ref, load_sem.at[6]),
        pltpu.make_async_copy(val_hbm, val_ref, load_sem.at[7]),
        pltpu.make_async_copy(prc_hbm, prc_ref, load_sem.at[8]),
        pltpu.make_async_copy(mp_hbm, mp_ref, load_sem.at[9]),
    ]
    for item in loads:
        item.start()

    barrier = pltpu.get_barrier_semaphore()
    group = [(dt, de) for dt in range(T) for de in range(E) if dt or de]

    def mate(dt, de):
        return {"tm": lax.rem(k + dt, T), "ens": lax.rem(e + de, E)}

    for dt, de in group:
        pl.semaphore_signal(barrier, inc=1, device_id=mate(dt, de), device_id_type=MESH)
    for db in range(1, L):
        pl.semaphore_signal(barrier, inc=1, device_id={"lat": lax.rem(b + db, L)}, device_id_type=MESH)

    def remote(src, dst, ssem, rsem, device):
        return pltpu.make_async_remote_copy(
            src_ref=src, dst_ref=dst, send_sem=ssem, recv_sem=rsem, device_id=device, device_id_type=MESH
        )

    up = {"lat": lax.rem(b + 1, L)}
    down = {"lat": lax.rem(b + L - 1, L)}
    later_dev = {"tm": lax.rem(k + 1, T)}
    prior_dev = {"tm": lax.rem(k + T - 1, T)}
    partner = {"ens": other}
    has_up, has_down = b < L - 1, b > 0
    has_later, has_prior = k < T - 1, k > 0

    for item in loads[:3]:
        item.wait()
    for at, ref in enumerate((inc_v, wlon_v, wlat_v)):
        for i in range(half):
            wide[at, i, 0:16, 0:lon] = ref[i]
            extend(wide, (at, i), lon)
            h_first[i, at] = wide[at, i, 0:4]
            h_last[i, at] = wide[at, i, crow - 4 : crow]

    pl.semaphore_wait(barrier, len(group) + L - 1)

    h_up = [remote(h_last.at[i], h_before.at[i], h_ssem.at[0, i], h_rsem.at[0, i], up) for i in range(half)]
    h_down = [remote(h_first.at[i], h_after.at[i], h_ssem.at[1, i], h_rsem.at[1, i], down) for i in range(half)]
    e_copy = [remote(end_v.at[i], prior_v.at[i], e_ssem.at[i], e_rsem.at[i], later_dev) for i in range(half)]
    n_copy = remote(inc_v, nxt_v, t_ssem.at[0], t_rsem.at[0], prior_dev)

    for i in range(half):
        @pl.when(has_up)
        def _():
            h_up[i].start()

        @pl.when(has_down)
        def _():
            h_down[i].start()

    @pl.when(has_prior)
    def _():
        n_copy.start()

    loads[4].wait()
    p_copy = remote(pert_v.at[e], pert_v.at[e], p_ssem, p_rsem, partner)
    p_copy.start()

    @pl.when(jnp.logical_not(has_up))
    def _():
        h_after[...] = jnp.zeros_like(h_after)
        a_after[...] = jnp.zeros_like(a_after)

    @pl.when(jnp.logical_not(has_down))
    def _():
        h_before[...] = jnp.zeros_like(h_before)
        a_before[...] = jnp.zeros_like(a_before)

    @pl.when(jnp.logical_not(has_prior))
    def _():
        prior_v[...] = jnp.zeros_like(prior_v)

    edge_in = ((e == 0) & has_down) | ((e == E - 1) & has_up)

    @pl.when(jnp.logical_not(edge_in))
    def _():
        edge_v[...] = jnp.zeros_like(edge_v)

    for item in loads[5:]:
        item.wait()
    loads[3].wait()
    jhi[:, width - 128 : width] = jnp.zeros((flat, 128), jnp.bfloat16)
    jlo[:, width - 128 : width] = jnp.zeros((flat, 128), jnp.bfloat16)

    def cut(at, carry):
        some = pl.ds(pl.multiple_of(at * 32, 32), 32)
        hi, lo = split(jac_v[some, :])
        jhi[some, 0:lon] = hi
        jlo[some, 0:lon] = lo
        return carry

    lax.fori_loop(0, flat // 32, cut, 0)

    column = lax.broadcasted_iota(jnp.int32, (blocks, flat), 1)
    block = lax.broadcasted_iota(jnp.int32, (blocks, flat), 0)
    mine = (column >= block * slots) & (column < (block + 1) * slots)
    spread = mine.astype(jnp.float32)
    first_column = lax.broadcasted_iota(jnp.int32, (1, flat), 1)
    slot = (first_column % slots).astype(jnp.float32)
    tile_slot = lax.broadcasted_iota(jnp.int32, (slots, flat), 0)
    tile_column = lax.broadcasted_iota(jnp.int32, (slots, flat), 1) % slots
    tiled = (tile_slot == tile_column).astype(jnp.float32)

    def flatten(ref):
        return jnp.sum(mm(ref[...], spread, NN, HIGHEST) * tiled, axis=0, keepdims=True)

    values, precisions = flatten(val_ref), flatten(prc_ref)
    counts = mm(jnp.broadcast_to(cnt_ref[...].astype(jnp.float32), (8, blocks)), spread, NN, HIGHEST)[0:1]
    rows = mm(jnp.broadcast_to(rows_ref[...].astype(jnp.float32), (8, blocks)), spread, NN, HIGHEST)[0:1]
    precisions = jnp.where(slot < counts - 0.5, precisions, 0.0)
    local = lax.broadcasted_iota(jnp.int32, (half * crow, flat), 0) + e * (half * crow)
    reads = (jnp.abs(rows - local.astype(jnp.float32)) < 0.5).astype(jnp.float32)

    for i in range(half):
        @pl.when(has_down)
        def _():
            h_up[i].wait_recv()

        @pl.when(has_up)
        def _():
            h_down[i].wait_recv()

        for at in range(3):
            wide[at, i, crow : crow + 4] = h_after[i, at]
            wide[at, i, crow + 4 : crow + 8] = h_before[i, at]
        wl, wt = wide[1, i], wide[2, i]
        wl2, wt2 = wl * wl, wt * wt
        coef[i, 0] = 1.0 - wl2 - wt2
        coef[i, 1] = 0.5 * (wl2 - wl)
        coef[i, 2] = 0.5 * (wl2 + wl)
        coef[i, 3] = 0.5 * (wt2 - wt)
        coef[i, 4] = 0.5 * (wt2 + wt)
        for _ in range(STEPS):
            f = wide[0, i]
            wide[0, i] = (
                coef[i, 0] * f
                + coef[i, 1] * turn(f, -1, 1)
                + coef[i, 2] * turn(f, 1, 1)
                + coef[i, 3] * turn(f, -1, 0)
                + coef[i, 4] * turn(f, 1, 0)
            )
        end_v[i] = wide[0, i, 0:crow]

        @pl.when(has_later & (i < half // 2))
        def _():
            e_copy[i].start()

    fhi, flo = split(jnp.concatenate([end_v[i] for i in range(half)], axis=0))
    jh, jl = jhi[...], jlo[...]
    rows_own = half * crow
    both = mm(jnp.concatenate([fhi, flo], axis=0), jh, NT)
    seen = both[:rows_own] + both[rows_own:] + mm(fhi, jl, NT)
    evolved = jnp.sum(seen * reads, axis=0, keepdims=True)
    whi, wlo = split(reads * (precisions * (evolved - values)))
    both = mm(jnp.concatenate([whi, wlo], axis=0), jh, NN)
    placed = both[:rows_own] + both[rows_own:] + mm(whi, jl, NN)

    @pl.when(has_later)
    def _():
        n_copy.wait_recv()

    @pl.when(jnp.logical_not(has_later))
    def _():
        for i in range(half):
            nxt_v[i] = end_v[i, :, 0:lon]

    for i in range(half):
        prec = mp_ref[e * half + i]
        later = prec * (nxt_v[i] - end_v[i, :, 0:lon])
        adj[i, 0:crow, 0:lon] = placed[i * crow : (i + 1) * crow, 0:lon] - later
        extend(adj, (i,), lon)
        adj[i, crow : crow + 8] = jnp.zeros((8, width), jnp.float32)

    def back(i):
        g = adj[i]
        return (
            coef[i, 0] * g
            + turn(coef[i, 1] * g, 1, 1)
            + turn(coef[i, 2] * g, -1, 1)
            + turn(coef[i, 3] * g, 1, 0)
            + turn(coef[i, 4] * g, -1, 0)
        )

    def owner_copy(i, h):
        return remote(
            forc.at[i, h], rs_v.at[k], rs_ssem.at[i, h], rs_rsem.at[k], {"tm": e * half + i, "ens": h}
        )

    def edge_copy(i, h, device):
        return remote(edge.at[i, h], edge_v.at[k], ed_ssem.at[i, h], ed_rsem.at[k], device)

    edge_up = [edge_copy(i, 0, {"tm": e * half + i, "lat": lax.rem(b + 1, L), "ens": 0}) for i in range(half)]
    edge_down = [
        edge_copy(i, 1, {"tm": e * half + i, "lat": lax.rem(b + L - 1, L), "ens": E - 1}) for i in range(half)
    ]

    for i in range(half):
        for h in range(E):
            forc[i, h] = adj[i, h * 8 : h * 8 + 8]
        rim = jnp.zeros((8, width), jnp.float32)
        for _ in range(STEPS - 1):
            adj[i] = back(i)
            for h in range(E):
                forc[i, h] += adj[i, h * 8 : h * 8 + 8]
            rim = rim + adj[i, crow : crow + 8]
        edge[i, 0] = rim[0:4]
        edge[i, 1] = rim[4:8]

        @pl.when(has_up)
        def _():
            edge_up[i].start()

        @pl.when(has_down)
        def _():
            edge_down[i].start()

        for h in range(E):
            here = (k == e * half + i) & (e == h)

            @pl.when(here)
            def _():
                rs_v[k] = forc[i, h]

            @pl.when(jnp.logical_not(here))
            def _():
                owner_copy(i, h).start()

    for i in range(half):
        adj[i] = back(i)
        a_up_v[i] = adj[i, crow : crow + 4]
        a_down_v[i] = adj[i, crow + 4 : crow + 8]
    a_up = remote(a_up_v, a_before, a_ssem.at[0], a_rsem.at[0], up)
    a_down = remote(a_down_v, a_after, a_ssem.at[1], a_rsem.at[1], down)

    @pl.when(has_up)
    def _():
        a_up.start()

    @pl.when(has_down)
    def _():
        a_down.start()

    for i in range(half):
        for h in range(E):
            here = (k == e * half + i) & (e == h)

            @pl.when(jnp.logical_not(here))
            def _():
                owner_copy(i, h).wait_send()

    @pl.when(has_later)
    def _():
        for i in range(half // 2, half):
            e_copy[i].start()

    p_copy.wait_recv()
    for at in range(T):
        inside = (k == at) & (e == at // half)

        @pl.when(jnp.logical_not(inside))
        def _():
            remote(forc.at[0, 0], rs_v.at[at], rs_ssem.at[0, 0], rs_rsem.at[at], partner).wait_recv()

    @pl.when(edge_in)
    def _():
        for at in range(T):
            remote(edge.at[0, 0], edge_v.at[at], ed_ssem.at[0, 0], ed_rsem.at[at], partner).wait_recv()

    total, rim = rs_v[0], edge_v[0]
    for at in range(1, T):
        total = total + rs_v[at]
        rim = rim + edge_v[at]
    line = lax.broadcasted_iota(jnp.int32, (8, width), 0)
    rim = jnp.concatenate([rim, rim], axis=0)
    total = total + jnp.where((line < 4) == (e == 0), rim, 0.0)
    total = total[:, 0:lon]
    lane = lax.broadcasted_iota(jnp.int32, (8, 128), 1)
    part = jnp.zeros((8, 128), jnp.float32)
    for m in range(E * members):
        dots = jnp.sum(pert_v[m // members, m % members, e] * total, axis=1, keepdims=True)
        part = jnp.where(lane == m, dots, part)
    ca_send[...] = part
    me = k * E + e
    ca_v[me] = part
    ca_copies = []
    for dt, de in group:
        copy = remote(ca_send, ca_v.at[me], ca_ssem.at[dt * E + de], ca_rsem.at[me], mate(dt, de))
        copy.start()
        ca_copies.append(copy)
    @pl.when(has_prior)
    def _():
        for i in range(half):
            e_copy[i].wait_recv()

    @pl.when(has_down)
    def _():
        a_up.wait_recv()

    @pl.when(has_up)
    def _():
        a_down.wait_recv()

    for i in range(half):
        prec = mp_ref[e * half + i]
        gap = jnp.zeros((crow - 8, lon), jnp.float32)
        rims = jnp.concatenate([a_before[i][:, 0:lon], gap, a_after[i][:, 0:lon]], axis=0)
        grad_v[e * half + i] = adj[i, 0:crow, 0:lon] + rims + prec * (inc_v[i] - prior_v[i, :, 0:lon])
    g_copy = remote(grad_v.at[own], grad_v.at[own], g_ssem, g_rsem, partner)
    g_copy.start()

    for dt, de in group:
        it = lax.rem(k + dt, T) * E + lax.rem(e + de, E)
        remote(ca_send, ca_v.at[it], ca_ssem.at[0], ca_rsem.at[it], partner).wait_recv()
    part = ca_v[0]
    for at in range(1, T * E):
        part = part + ca_v[at]
    cb_send[...] = part
    cb_v[b] = part
    cb_copies = []
    for db in range(1, L):
        copy = remote(cb_send, cb_v.at[b], cb_ssem.at[db], cb_rsem.at[b], {"lat": lax.rem(b + db, L)})
        copy.start()
        cb_copies.append(copy)

    g_copy.wait_recv()
    for db in range(1, L):
        it = lax.rem(b + db, L)
        remote(cb_send, cb_v.at[it], cb_ssem.at[0], cb_rsem.at[it], partner).wait_recv()
    @pl.when(has_up)
    def _():
        for i in range(half):
            h_up[i].wait_send()
        a_up.wait_send()

    @pl.when(has_down)
    def _():
        for i in range(half):
            h_down[i].wait_send()
        a_down.wait_send()

    @pl.when(has_prior)
    def _():
        n_copy.wait_send()

    @pl.when(has_later)
    def _():
        for i in range(half):
            e_copy[i].wait_send()

    p_copy.wait_send()
    g_copy.wait_send()
    for i in range(half):
        @pl.when(has_up)
        def _():
            edge_up[i].wait_send()

        @pl.when(has_down)
        def _():
            edge_down[i].wait_send()

    for copy in ca_copies + cb_copies:
        copy.wait_send()


def finish(L, grad_v, pert_v, cb_v, grad_hbm, step_hbm, step_v, out_sem):
    g_out = pltpu.make_async_copy(grad_v, grad_hbm, out_sem.at[0])
    g_out.start()
    ens, members, rows, _, lon = pert_v.shape
    count = ens * members
    part = cb_v[0]
    for at in range(1, L):
        part = part + cb_v[at]
    factor = jnp.broadcast_to(jnp.sum(part, axis=0, keepdims=True), (8, 128)) * (-1.0 / (count - 1.0))
    for h in range(rows):
        mixed = jnp.zeros((8, lon), jnp.float32)
        for m in range(count):
            mixed = mixed + factor[:, m : m + 1] * pert_v[m // members, m % members, h]
        step_v[h * 8 : h * 8 + 8, :] = mixed
    s_out = pltpu.make_async_copy(step_v, step_hbm, out_sem.at[1])
    s_out.start()
    g_out.wait()
    s_out.wait()


def on_device(T, L, E, increment, wind_lon, wind_lat, model_precision, perturbations, obs_rows, obs_jacobian,
              obs_values, obs_precision, obs_counts):
    _, levels, crow, lon = increment.shape
    members = perturbations.shape[0]
    blocks, slots = obs_jacobian.shape[1:3]
    half, width = levels // E, -(-lon // 128) * 128
    flat = blocks * slots
    f32, dma = jnp.float32, pltpu.SemaphoreType.DMA
    vmem, anyw = pl.BlockSpec(memory_space=pltpu.VMEM), pl.BlockSpec(memory_space=pl.ANY)

    def buf(*shape, kind=f32):
        return pltpu.VMEM(shape, kind)

    parts = pl.pallas_call(
        functools.partial(kernel, T, L, E),
        out_shape=(
            buf(levels, crow, lon),
            buf(E, members, crow // 8, 8, lon),
            buf(L, 8, 128),
        ),
        in_specs=[pl.BlockSpec(memory_space=pltpu.HBM)] * 10,
        out_specs=(vmem, vmem, vmem),
        scratch_shapes=[
            pltpu.VMEM((1, blocks), jnp.int32), pltpu.VMEM((1, blocks), jnp.int32),
            buf(slots, blocks), buf(slots, blocks), pltpu.SMEM((levels,), f32),
            buf(half, crow, lon), buf(half, crow, lon), buf(half, crow, lon),
            buf(flat, lon),
            buf(flat, width, kind=jnp.bfloat16), buf(flat, width, kind=jnp.bfloat16),
            buf(3, half, 24, width), buf(half, 5, 24, width), buf(half, 24, width),
            buf(half, 3, 4, width), buf(half, 3, 4, width), buf(half, 3, 4, width), buf(half, 3, 4, width),
            buf(half, 4, width), buf(half, 4, width), buf(half, 4, width), buf(half, 4, width),
            buf(half, crow, width), buf(half, crow, lon), buf(half, crow, width),
            buf(half, E, 8, width), buf(half, 2, 4, width), buf(T, 8, width), buf(T, 4, width),
            buf(8, 128), buf(T * E, 8, 128), buf(8, 128),
            dma((10,)), dma((2, half)), dma((2, half)), dma((2,)), dma((2,)), dma((1,)), dma((1,)),
            dma((half,)), dma((half,)), dma, dma,
            dma((half, E)), dma((T,)), dma((half, 2)), dma((T,)),
            dma((T * E,)), dma((T * E,)), dma((L,)), dma((L,)), dma, dma,
        ],
        compiler_params=pltpu.CompilerParams(
            collective_id=0, has_side_effects=True, vmem_limit_bytes=56 * 1024 * 1024
        ),
    )(
        obs_rows, obs_counts, obs_values[0].T, obs_precision[0].T, model_precision,
        increment[0], wind_lon[0], wind_lat[0],
        obs_jacobian.reshape(flat, lon),
        perturbations.reshape(members, crow // 8, 8, lon),
    )
    grad, step = pl.pallas_call(
        functools.partial(finish, L),
        out_shape=(
            jax.ShapeDtypeStruct((levels, crow, lon), f32),
            jax.ShapeDtypeStruct((crow, lon), f32),
        ),
        in_specs=[vmem] * 3,
        out_specs=(anyw, anyw),
        scratch_shapes=[buf(crow, lon), dma((2,))],
        compiler_params=pltpu.CompilerParams(vmem_limit_bytes=8 * 1024 * 1024),
    )(*[pltpu.with_memory_space_constraint(item, pltpu.VMEM) for item in parts])
    return grad[None], step[None]


def solution(mesh):
    T, L, E = mesh.shape["tm"], mesh.shape["lat"], mesh.shape["ens"]
    placed = (
        P("tm", None, "lat", None),
        P("tm", None, "lat", None),
        P("tm", None, "lat", None),
        P(),
        P("ens", "tm", "lat", None),
        P("tm", "lat"),
        P("tm", "lat", None, None),
        P("tm", "lat", None),
        P("tm", "lat", None),
        P("tm", "lat"),
    )
    return jax.shard_map(
        functools.partial(on_device, T, L, E),
        mesh=mesh,
        in_specs=placed,
        out_specs=(P("tm", None, "lat", None), P("tm", "lat", None)),
        check_vma=False,
    )
```

```python
import functools

import jax
import jax.numpy as jnp
from jax import lax
from jax.experimental import pallas as pl
from jax.experimental.pallas import tpu as pltpu
from jax.sharding import PartitionSpec as P

STEPS = 4
MESH = pl.DeviceIdType.MESH
HIGHEST = lax.Precision.HIGHEST
NT = (((1,), (1,)), ((), ()))
NN = (((1,), (0,)), ((), ()))


def mm(a, b, dims, precision=None):
    return lax.dot_general(a, b, dims, precision=precision, preferred_element_type=jnp.float32)


def split(value):
    hi = value.astype(jnp.bfloat16)
    lo = (value - hi.astype(jnp.float32)).astype(jnp.bfloat16)
    return hi, lo


def turn(value, steps, axis):
    return pltpu.roll(value, steps % value.shape[axis], axis)


def extend(ref, where, lon):
    width = ref.shape[-1]
    rem = lon % 128
    last = ref[where + (slice(0, 16), slice(width - 128, width))]
    before = ref[where + (slice(0, 16), slice(width - 256, width - 128))]
    first = ref[where + (slice(0, 16), slice(0, 128))]
    lane = lax.broadcasted_iota(jnp.int32, last.shape, 1)
    wrapped = jnp.where(lane < 128 - rem, turn(before, 128 - rem, 1), turn(last, 128 - rem, 1))
    right = jnp.where(lane < rem + (128 - rem) // 2, turn(first, rem, 1), wrapped)
    ref[where + (slice(0, 16), slice(width - 128, width))] = jnp.where(lane < rem, last, right)


def kernel(
    T, L, E,
    rows_hbm, cnt_hbm, val_hbm, prc_hbm, mp_hbm, inc_hbm, wlon_hbm, wlat_hbm, jac_hbm, pert_hbm,
    grad_v, pert_v, cb_v,
    rows_ref, cnt_ref, val_ref, prc_ref, mp_ref, inc_v, wlon_v, wlat_v, jac_v, jhi, jlo, wide, coef, adj,
    h_first, h_last, h_after, h_before, a_up_v, a_down_v, a_after, a_before,
    end_v, nxt_v, prior_v, forc, edge, rs_v, edge_v, ca_send, ca_v, cb_send,
    load_sem, h_ssem, h_rsem, a_ssem, a_rsem, t_ssem, t_rsem, e_ssem, e_rsem, p_ssem, p_rsem,
    rs_ssem, rs_rsem, ed_ssem, ed_rsem, ca_ssem, ca_rsem, cb_ssem, cb_rsem, g_ssem, g_rsem, all_sem,
):
    k, b, e = lax.axis_index("tm"), lax.axis_index("lat"), lax.axis_index("ens")
    half, crow, lon = inc_v.shape
    width = wide.shape[-1]
    members = pert_v.shape[1]
    slots, blocks = val_ref.shape
    flat = blocks * slots
    other = 1 - e
    own = pl.ds(e * half, half)

    loads = [
        pltpu.make_async_copy(inc_hbm.at[own], inc_v, load_sem.at[0]),
        pltpu.make_async_copy(wlon_hbm.at[own], wlon_v, load_sem.at[1]),
        pltpu.make_async_copy(wlat_hbm.at[own], wlat_v, load_sem.at[2]),
        pltpu.make_async_copy(jac_hbm, jac_v, load_sem.at[3]),
        pltpu.make_async_copy(pert_hbm, pert_v.at[e], load_sem.at[4]),
        pltpu.make_async_copy(rows_hbm, rows_ref, load_sem.at[5]),
        pltpu.make_async_copy(cnt_hbm, cnt_ref, load_sem.at[6]),
        pltpu.make_async_copy(val_hbm, val_ref, load_sem.at[7]),
        pltpu.make_async_copy(prc_hbm, prc_ref, load_sem.at[8]),
        pltpu.make_async_copy(mp_hbm, mp_ref, load_sem.at[9]),
    ]
    for item in loads[:3]:
        item.start()

    barrier = pltpu.get_barrier_semaphore()
    direct = T * L * E <= 64
    group = [(dt, de) for dt in range(T) for de in range(E) if dt or de]

    def mate(dt, de):
        return {"tm": lax.rem(k + dt, T), "ens": lax.rem(e + de, E)}

    for dt, de in group:
        pl.semaphore_signal(barrier, inc=1, device_id=mate(dt, de), device_id_type=MESH)
    for db in range(1, L):
        pl.semaphore_signal(barrier, inc=1, device_id={"lat": lax.rem(b + db, L)}, device_id_type=MESH)

    def remote(src, dst, ssem, rsem, device):
        return pltpu.make_async_remote_copy(
            src_ref=src, dst_ref=dst, send_sem=ssem, recv_sem=rsem, device_id=device, device_id_type=MESH
        )

    up = {"lat": lax.rem(b + 1, L)}
    down = {"lat": lax.rem(b + L - 1, L)}
    later_dev = {"tm": lax.rem(k + 1, T)}
    prior_dev = {"tm": lax.rem(k + T - 1, T)}
    partner = {"ens": other}
    has_up, has_down = b < L - 1, b > 0
    has_later, has_prior = k < T - 1, k > 0

    for item in loads[:3]:
        item.wait()
    for item in loads[4:5] + loads[3:4] + loads[5:]:
        item.start()
    for at, ref in enumerate((inc_v, wlon_v, wlat_v)):
        for i in range(half):
            wide[at, i, 0:16, 0:lon] = ref[i]
            extend(wide, (at, i), lon)
            h_first[i, at] = wide[at, i, 0:4]
            h_last[i, at] = wide[at, i, crow - 4 : crow]

    pl.semaphore_wait(barrier, len(group) + L - 1)
    if direct:
        for db in range(1, L):
            pl.semaphore_signal(all_sem, inc=1, device_id={"lat": lax.rem(b + db, L)}, device_id_type=MESH)

    h_up = [remote(h_last.at[i], h_before.at[i], h_ssem.at[0, i], h_rsem.at[0, i], up) for i in range(half)]
    h_down = [remote(h_first.at[i], h_after.at[i], h_ssem.at[1, i], h_rsem.at[1, i], down) for i in range(half)]
    e_copy = [remote(end_v.at[i], prior_v.at[i], e_ssem.at[i], e_rsem.at[i], later_dev) for i in range(half)]
    n_copy = remote(inc_v, nxt_v, t_ssem.at[0], t_rsem.at[0], prior_dev)

    for i in range(half):
        @pl.when(has_up)
        def _():
            h_up[i].start()

        @pl.when(has_down)
        def _():
            h_down[i].start()

    @pl.when(has_prior)
    def _():
        n_copy.start()

    loads[4].wait()
    p_copy = remote(pert_v.at[e], pert_v.at[e], p_ssem, p_rsem, partner)
    p_copy.start()

    @pl.when(jnp.logical_not(has_up))
    def _():
        h_after[...] = jnp.zeros_like(h_after)
        a_after[...] = jnp.zeros_like(a_after)

    @pl.when(jnp.logical_not(has_down))
    def _():
        h_before[...] = jnp.zeros_like(h_before)
        a_before[...] = jnp.zeros_like(a_before)

    @pl.when(jnp.logical_not(has_prior))
    def _():
        prior_v[...] = jnp.zeros_like(prior_v)

    edge_in = ((e == 0) & has_down) | ((e == E - 1) & has_up)

    @pl.when(jnp.logical_not(edge_in))
    def _():
        edge_v[...] = jnp.zeros_like(edge_v)

    for item in loads[5:]:
        item.wait()
    loads[3].wait()
    jhi[:, width - 128 : width] = jnp.zeros((flat, 128), jnp.bfloat16)
    jlo[:, width - 128 : width] = jnp.zeros((flat, 128), jnp.bfloat16)

    def cut(at, carry):
        some = pl.ds(pl.multiple_of(at * 32, 32), 32)
        hi, lo = split(jac_v[some, :])
        jhi[some, 0:lon] = hi
        jlo[some, 0:lon] = lo
        return carry

    lax.fori_loop(0, flat // 32, cut, 0)

    column = lax.broadcasted_iota(jnp.int32, (blocks, flat), 1)
    block = lax.broadcasted_iota(jnp.int32, (blocks, flat), 0)
    mine = (column >= block * slots) & (column < (block + 1) * slots)
    spread = mine.astype(jnp.float32)
    first_column = lax.broadcasted_iota(jnp.int32, (1, flat), 1)
    slot = (first_column % slots).astype(jnp.float32)
    tile_slot = lax.broadcasted_iota(jnp.int32, (slots, flat), 0)
    tile_column = lax.broadcasted_iota(jnp.int32, (slots, flat), 1) % slots
    tiled = (tile_slot == tile_column).astype(jnp.float32)

    def flatten(ref):
        return jnp.sum(mm(ref[...], spread, NN, HIGHEST) * tiled, axis=0, keepdims=True)

    values, precisions = flatten(val_ref), flatten(prc_ref)
    counts = mm(jnp.broadcast_to(cnt_ref[...].astype(jnp.float32), (8, blocks)), spread, NN, HIGHEST)[0:1]
    rows = mm(jnp.broadcast_to(rows_ref[...].astype(jnp.float32), (8, blocks)), spread, NN, HIGHEST)[0:1]
    precisions = jnp.where(slot < counts - 0.5, precisions, 0.0)
    local = lax.broadcasted_iota(jnp.int32, (half * crow, flat), 0) + e * (half * crow)
    reads = (jnp.abs(rows - local.astype(jnp.float32)) < 0.5).astype(jnp.float32)

    for i in range(half):
        @pl.when(has_down)
        def _():
            h_up[i].wait_recv()

        @pl.when(has_up)
        def _():
            h_down[i].wait_recv()

        for at in range(3):
            wide[at, i, crow : crow + 4] = h_after[i, at]
            wide[at, i, crow + 4 : crow + 8] = h_before[i, at]
        wl, wt = wide[1, i], wide[2, i]
        wl2, wt2 = wl * wl, wt * wt
        coef[i, 0] = 1.0 - wl2 - wt2
        coef[i, 1] = 0.5 * (wl2 - wl)
        coef[i, 2] = 0.5 * (wl2 + wl)
        coef[i, 3] = 0.5 * (wt2 - wt)
        coef[i, 4] = 0.5 * (wt2 + wt)
        for _ in range(STEPS):
            f = wide[0, i]
            wide[0, i] = (
                coef[i, 0] * f
                + coef[i, 1] * turn(f, -1, 1)
                + coef[i, 2] * turn(f, 1, 1)
                + coef[i, 3] * turn(f, -1, 0)
                + coef[i, 4] * turn(f, 1, 0)
            )
        end_v[i] = wide[0, i, 0:crow]

        @pl.when(has_later & (i < half // 2))
        def _():
            e_copy[i].start()

    fhi, flo = split(jnp.concatenate([end_v[i] for i in range(half)], axis=0))
    jh, jl = jhi[...], jlo[...]
    rows_own = half * crow
    both = mm(jnp.concatenate([fhi, flo], axis=0), jh, NT)
    seen = both[:rows_own] + both[rows_own:] + mm(fhi, jl, NT)
    evolved = jnp.sum(seen * reads, axis=0, keepdims=True)
    whi, wlo = split(reads * (precisions * (evolved - values)))
    both = mm(jnp.concatenate([whi, wlo], axis=0), jh, NN)
    placed = both[:rows_own] + both[rows_own:] + mm(whi, jl, NN)

    @pl.when(has_later)
    def _():
        n_copy.wait_recv()

    @pl.when(jnp.logical_not(has_later))
    def _():
        for i in range(half):
            nxt_v[i] = end_v[i, :, 0:lon]

    for i in range(half):
        prec = mp_ref[e * half + i]
        later = prec * (nxt_v[i] - end_v[i, :, 0:lon])
        adj[i, 0:crow, 0:lon] = placed[i * crow : (i + 1) * crow, 0:lon] - later
        extend(adj, (i,), lon)
        adj[i, crow : crow + 8] = jnp.zeros((8, width), jnp.float32)

    def back(i):
        g = adj[i]
        return (
            coef[i, 0] * g
            + turn(coef[i, 1] * g, 1, 1)
            + turn(coef[i, 2] * g, -1, 1)
            + turn(coef[i, 3] * g, 1, 0)
            + turn(coef[i, 4] * g, -1, 0)
        )

    def owner_copy(i, h):
        return remote(
            forc.at[i, h], rs_v.at[k], rs_ssem.at[i, h], rs_rsem.at[k], {"tm": e * half + i, "ens": h}
        )

    def edge_copy(i, h, device):
        return remote(edge.at[i, h], edge_v.at[k], ed_ssem.at[i, h], ed_rsem.at[k], device)

    edge_up = [edge_copy(i, 0, {"tm": e * half + i, "lat": lax.rem(b + 1, L), "ens": 0}) for i in range(half)]
    edge_down = [
        edge_copy(i, 1, {"tm": e * half + i, "lat": lax.rem(b + L - 1, L), "ens": E - 1}) for i in range(half)
    ]

    for i in range(half):
        for h in range(E):
            forc[i, h] = adj[i, h * 8 : h * 8 + 8]
        rim = jnp.zeros((8, width), jnp.float32)
        for _ in range(STEPS - 1):
            adj[i] = back(i)
            for h in range(E):
                forc[i, h] += adj[i, h * 8 : h * 8 + 8]
            rim = rim + adj[i, crow : crow + 8]
        edge[i, 0] = rim[0:4]
        edge[i, 1] = rim[4:8]

        @pl.when(has_up)
        def _():
            edge_up[i].start()

        @pl.when(has_down)
        def _():
            edge_down[i].start()

        for h in range(E):
            here = (k == e * half + i) & (e == h)

            @pl.when(here)
            def _():
                rs_v[k] = forc[i, h]

            @pl.when(jnp.logical_not(here))
            def _():
                owner_copy(i, h).start()

    for i in range(half):
        adj[i] = back(i)
        a_up_v[i] = adj[i, crow : crow + 4]
        a_down_v[i] = adj[i, crow + 4 : crow + 8]
    a_up = remote(a_up_v, a_before, a_ssem.at[0], a_rsem.at[0], up)
    a_down = remote(a_down_v, a_after, a_ssem.at[1], a_rsem.at[1], down)

    @pl.when(has_up)
    def _():
        a_up.start()

    @pl.when(has_down)
    def _():
        a_down.start()

    for i in range(half):
        for h in range(E):
            here = (k == e * half + i) & (e == h)

            @pl.when(jnp.logical_not(here))
            def _():
                owner_copy(i, h).wait_send()

    @pl.when(has_later)
    def _():
        for i in range(half // 2, half):
            e_copy[i].start()

    p_copy.wait_recv()
    for at in range(T):
        inside = (k == at) & (e == at // half)

        @pl.when(jnp.logical_not(inside))
        def _():
            remote(forc.at[0, 0], rs_v.at[at], rs_ssem.at[0, 0], rs_rsem.at[at], partner).wait_recv()

    @pl.when(edge_in)
    def _():
        for at in range(T):
            remote(edge.at[0, 0], edge_v.at[at], ed_ssem.at[0, 0], ed_rsem.at[at], partner).wait_recv()

    total, rim = rs_v[0], edge_v[0]
    for at in range(1, T):
        total = total + rs_v[at]
        rim = rim + edge_v[at]
    line = lax.broadcasted_iota(jnp.int32, (8, width), 0)
    rim = jnp.concatenate([rim, rim], axis=0)
    total = total + jnp.where((line < 4) == (e == 0), rim, 0.0)
    total = total[:, 0:lon]
    lane = lax.broadcasted_iota(jnp.int32, (8, 128), 1)
    part = jnp.zeros((8, 128), jnp.float32)
    for m in range(E * members):
        dots = jnp.sum(pert_v[m // members, m % members, e] * total, axis=1, keepdims=True)
        part = jnp.where(lane == m, dots, part)
    part = jnp.sum(part, axis=0, keepdims=True)
    ca_send[...] = part
    if direct:
        crowd = [(dt, db, de) for dt in range(T) for db in range(L) for de in range(E) if dt or db or de]
        pl.semaphore_wait(all_sem, L - 1)
    else:
        crowd = [(dt, 0, de) for dt, de in group]

    def seat(dt, db, de):
        at, lat, ens = lax.rem(k + dt, T), lax.rem(b + db, L), lax.rem(e + de, E)
        index = (at * L + lat) * E + ens if direct else at * E + ens
        return index, {"tm": at, "lat": lat, "ens": ens}

    sums = cb_v if direct else ca_v
    me, _ = seat(0, 0, 0)
    sums[me] = part
    coef_copies = []
    for at, (dt, db, de) in enumerate(crowd):
        copy = remote(ca_send, sums.at[me], ca_ssem.at[at], ca_rsem.at[me], seat(dt, db, de)[1])
        copy.start()
        coef_copies.append(copy)

    @pl.when(has_prior)
    def _():
        for i in range(half):
            e_copy[i].wait_recv()

    @pl.when(has_down)
    def _():
        a_up.wait_recv()

    @pl.when(has_up)
    def _():
        a_down.wait_recv()

    for i in range(half):
        prec = mp_ref[e * half + i]
        gap = jnp.zeros((crow - 8, lon), jnp.float32)
        rims = jnp.concatenate([a_before[i][:, 0:lon], gap, a_after[i][:, 0:lon]], axis=0)
        grad_v[e * half + i] = adj[i, 0:crow, 0:lon] + rims + prec * (inc_v[i] - prior_v[i, :, 0:lon])
    g_copy = remote(grad_v.at[own], grad_v.at[own], g_ssem, g_rsem, partner)
    g_copy.start()
    for dt, db, de in crowd:
        it, _ = seat(dt, db, de)
        remote(ca_send, sums.at[it], ca_ssem.at[0], ca_rsem.at[it], partner).wait_recv()
    if not direct:
        part = ca_v[0]
        for at in range(1, T * E):
            part = part + ca_v[at]
        cb_send[...] = part
        cb_v[b] = part
        for db in range(1, L):
            copy = remote(cb_send, cb_v.at[b], cb_ssem.at[db], cb_rsem.at[b], {"lat": lax.rem(b + db, L)})
            copy.start()
            coef_copies.append(copy)
        for db in range(1, L):
            it = lax.rem(b + db, L)
            remote(cb_send, cb_v.at[it], cb_ssem.at[0], cb_rsem.at[it], partner).wait_recv()
    g_copy.wait_recv()

    @pl.when(has_up)
    def _():
        for i in range(half):
            h_up[i].wait_send()
        a_up.wait_send()

    @pl.when(has_down)
    def _():
        for i in range(half):
            h_down[i].wait_send()
        a_down.wait_send()

    @pl.when(has_prior)
    def _():
        n_copy.wait_send()

    @pl.when(has_later)
    def _():
        for i in range(half):
            e_copy[i].wait_send()

    p_copy.wait_send()
    g_copy.wait_send()
    for i in range(half):
        @pl.when(has_up)
        def _():
            edge_up[i].wait_send()

        @pl.when(has_down)
        def _():
            edge_down[i].wait_send()

    for copy in coef_copies:
        copy.wait_send()


def finish(grad_v, pert_v, cb_v, grad_hbm, step_hbm, step_v, out_sem):
    g_out = pltpu.make_async_copy(grad_v, grad_hbm, out_sem.at[0])
    g_out.start()
    ens, members, rows, _, lon = pert_v.shape
    count = ens * members
    part = cb_v[0]
    for at in range(1, cb_v.shape[0]):
        part = part + cb_v[at]
    factor = jnp.broadcast_to(part, (8, 128)) * (-1.0 / (count - 1.0))
    for h in range(rows):
        mixed = jnp.zeros((8, lon), jnp.float32)
        for m in range(count):
            mixed = mixed + factor[:, m : m + 1] * pert_v[m // members, m % members, h]
        step_v[h * 8 : h * 8 + 8, :] = mixed
    s_out = pltpu.make_async_copy(step_v, step_hbm, out_sem.at[1])
    s_out.start()
    g_out.wait()
    s_out.wait()


def on_device(T, L, E, increment, wind_lon, wind_lat, model_precision, perturbations, obs_rows, obs_jacobian,
              obs_values, obs_precision, obs_counts):
    _, levels, crow, lon = increment.shape
    members = perturbations.shape[0]
    blocks, slots = obs_jacobian.shape[1:3]
    half, width = levels // E, -(-lon // 128) * 128
    flat = blocks * slots
    heard, spoken = (T * L * E, T * L * E) if T * L * E <= 64 else (L, T * E)
    f32, dma = jnp.float32, pltpu.SemaphoreType.DMA
    vmem, anyw = pl.BlockSpec(memory_space=pltpu.VMEM), pl.BlockSpec(memory_space=pl.ANY)

    def buf(*shape, kind=f32):
        return pltpu.VMEM(shape, kind)

    parts = pl.pallas_call(
        functools.partial(kernel, T, L, E),
        out_shape=(
            buf(levels, crow, lon),
            buf(E, members, crow // 8, 8, lon),
            buf(heard, 1, 128),
        ),
        in_specs=[pl.BlockSpec(memory_space=pltpu.HBM)] * 10,
        out_specs=(vmem, vmem, vmem),
        scratch_shapes=[
            pltpu.VMEM((1, blocks), jnp.int32), pltpu.VMEM((1, blocks), jnp.int32),
            buf(slots, blocks), buf(slots, blocks), pltpu.SMEM((levels,), f32),
            buf(half, crow, lon), buf(half, crow, lon), buf(half, crow, lon),
            buf(flat, lon),
            buf(flat, width, kind=jnp.bfloat16), buf(flat, width, kind=jnp.bfloat16),
            buf(3, half, 24, width), buf(half, 5, 24, width), buf(half, 24, width),
            buf(half, 3, 4, width), buf(half, 3, 4, width), buf(half, 3, 4, width), buf(half, 3, 4, width),
            buf(half, 4, width), buf(half, 4, width), buf(half, 4, width), buf(half, 4, width),
            buf(half, crow, width), buf(half, crow, lon), buf(half, crow, width),
            buf(half, E, 8, width), buf(half, 2, 4, width), buf(T, 8, width), buf(T, 4, width),
            buf(1, 128), buf(T * E, 1, 128), buf(1, 128),
            dma((10,)), dma((2, half)), dma((2, half)), dma((2,)), dma((2,)), dma((1,)), dma((1,)),
            dma((half,)), dma((half,)), dma, dma,
            dma((half, E)), dma((T,)), dma((half, 2)), dma((T,)),
            dma((spoken,)), dma((spoken,)), dma((L,)), dma((L,)), dma, dma, pltpu.SemaphoreType.REGULAR,
        ],
        compiler_params=pltpu.CompilerParams(
            collective_id=0, has_side_effects=True, vmem_limit_bytes=56 * 1024 * 1024
        ),
    )(
        obs_rows, obs_counts, obs_values[0].T, obs_precision[0].T, model_precision,
        increment[0], wind_lon[0], wind_lat[0],
        obs_jacobian.reshape(flat, lon),
        perturbations.reshape(members, crow // 8, 8, lon),
    )
    grad, step = pl.pallas_call(
        finish,
        out_shape=(
            jax.ShapeDtypeStruct((levels, crow, lon), f32),
            jax.ShapeDtypeStruct((crow, lon), f32),
        ),
        in_specs=[vmem] * 3,
        out_specs=(anyw, anyw),
        scratch_shapes=[buf(crow, lon), dma((2,))],
        compiler_params=pltpu.CompilerParams(vmem_limit_bytes=8 * 1024 * 1024),
    )(*[pltpu.with_memory_space_constraint(item, pltpu.VMEM) for item in parts])
    return grad[None], step[None]


def solution(mesh):
    T, L, E = mesh.shape["tm"], mesh.shape["lat"], mesh.shape["ens"]
    placed = (
        P("tm", None, "lat", None),
        P("tm", None, "lat", None),
        P("tm", None, "lat", None),
        P(),
        P("ens", "tm", "lat", None),
        P("tm", "lat"),
        P("tm", "lat", None, None),
        P("tm", "lat", None),
        P("tm", "lat", None),
        P("tm", "lat"),
    )
    return jax.shard_map(
        functools.partial(on_device, T, L, E),
        mesh=mesh,
        in_specs=placed,
        out_specs=(P("tm", None, "lat", None), P("tm", "lat", None)),
        check_vma=False,
    )
```
